16 devices in a mesh: frag: 4 (over z, y), dev: 4 (over x, core).
Axes of the slice: x: 2, y: 2, z: 2, core: 2. Of those that a mesh axis runs over, the one named last changes fastest.
Arguments:
- a_ints: bfloat16 [448, 112, 112, 112], P(('frag', 'dev')), parts along dimension 0
- c_occ: bfloat16 [448, 64], P('frag'), parts along dimension 0
- c_vir: bfloat16 [448, 32], P('frag'), parts along dimension 0
- eps_occ: float32 [256], P('frag'), parts along dimension 0
- eps_vir: float32 [128], P('frag'), parts along dimension 0
Outputs:
- output: float32 [256, 64], P('frag', 'dev'), parts along dimension 0
There are 4 independent parts. The reference program is written for one: setup_inputs(seed, part) draws one part's arguments, and reference() takes and returns one part's arrays. A program takes and returns all parts, laid end to end along the dimension named above; each array names one.
All inputs are finite; a program needn't handle non-finite values.
Results may differ from the reference program's by a relative error of at most 0.001.
Values are sent between devices in bfloat16 or wider.
A program may use at most 1 GiB of HBM per device.

```python
import jax
import jax.numpy as jnp
from jax import lax

PAD_BASIS = 112
NUM_OCC = 64
NUM_VIRT = 32


def setup_inputs(seed: int = 0, part: int = 0) -> dict:
    key_base = jax.random.fold_in(jax.random.key(seed), part)
    key_ints, key_occ, key_vir, key_eocc, key_evir = jax.random.split(key_base, 5)

    def draw_row(row_idx):
        raw_row = jax.random.normal(jax.random.fold_in(key_ints, row_idx), (PAD_BASIS, PAD_BASIS, PAD_BASIS), jnp.float32)
        mixed_row = (raw_row + 0.5 * jnp.transpose(raw_row, (2, 1, 0))) * (1.25 ** -0.5)
        return mixed_row.astype(jnp.bfloat16)

    a_ints = lax.map(draw_row, jnp.arange(PAD_BASIS))
    c_occ = (jax.random.normal(key_occ, (PAD_BASIS, NUM_OCC), jnp.float32) * PAD_BASIS ** -0.5).astype(jnp.bfloat16)
    c_vir = (jax.random.normal(key_vir, (PAD_BASIS, NUM_VIRT), jnp.float32) * (PAD_BASIS * NUM_VIRT) ** -0.5).astype(jnp.bfloat16)
    eps_occ = jax.random.uniform(key_eocc, (NUM_OCC,), jnp.float32, -1.5, -0.5)
    eps_vir = jax.random.uniform(key_evir, (NUM_VIRT,), jnp.float32, 0.3, 2.0)
    return {"a_ints": a_ints, "c_occ": c_occ, "c_vir": c_vir, "eps_occ": eps_occ, "eps_vir": eps_vir}


def reference(a_ints, c_occ, c_vir, eps_occ, eps_vir):
    occ_32 = c_occ.astype(jnp.float32)
    vir_32 = c_vir.astype(jnp.float32)

    def first_half(a_row):
        t_one = jnp.einsum("qrs,rj->qsj", a_row.astype(jnp.float32), occ_32).astype(jnp.bfloat16)
        return jnp.einsum("qsj,sb->qjb", t_one.astype(jnp.float32), vir_32).astype(jnp.bfloat16)

    half_mo = lax.map(first_half, a_ints)
    g_mat = jnp.einsum("pqjb,qa->pjba", half_mo.astype(jnp.float32), vir_32).astype(jnp.bfloat16)
    v_mo = jnp.einsum("pjba,pi->jbai", g_mat.astype(jnp.float32), occ_32)
    v_swap = jnp.swapaxes(v_mo, 1, 2)
    denominator = (eps_occ[:, None, None, None] + eps_occ[None, None, None, :]
                   - eps_vir[None, :, None, None] - eps_vir[None, None, :, None])
    pair_ji = jnp.sum(v_mo * (2.0 * v_mo - v_swap) / denominator, axis=(1, 2))
    return pair_ji.T
```

```python
import functools

import jax
import jax.numpy as jnp
from jax import lax
from jax.experimental import pallas as pl
from jax.experimental.pallas import tpu as pltpu
from jax.sharding import PartitionSpec as P

BF = jnp.bfloat16
F32 = jnp.float32
LANES = 128
GROUP_Q = 8
HALF_B = 16
PITCH = 40


def iota(shape, dim):
    return lax.broadcasted_iota(jnp.int32, shape, dim)


def dot32(a, b):
    return jnp.dot(a, b, preferred_element_type=F32)


def kernel(dims, eo_s, ev_s, eo_ref, cot_ref, cv_ref, a_hbm, out_ref,
           abuf, t0, t1, h0, h1, w2, w3, b4, gbuf, recv, vbuf, evc,
           a_sem, send_sem, recv_sem):
    rows, n, o, v, ndev = dims
    oj = o // ndev
    groups = n // GROUP_Q
    nb_hi = v // HALF_B
    half_cols = HALF_B * v
    me = lax.axis_index("dev")
    partner = me + 1 - 2 * (me % 2)
    peers = ((me + 2) % 4, (partner + 2) % 4, partner)

    def a_copy(p):
        slot = p % 3
        return pltpu.make_async_copy(a_hbm.at[p], abuf.at[slot], a_sem.at[slot])

    a_copy(0).start()
    a_copy(1).start()

    barrier = pltpu.get_barrier_semaphore()
    for d in peers:
        pl.semaphore_signal(barrier, inc=1, device_id={"dev": d},
                            device_id_type=pl.DeviceIdType.MESH)

    cv = cv_ref[...]
    col_b = (iota((v, 2 * LANES), 1) // LANES) * HALF_B + iota((v, 2 * LANES), 1) % HALF_B
    cvt = dot32(cv, jnp.where(iota((v, 2 * LANES), 0) == col_b, 1.0, 0.0).astype(BF))
    lane_q = (iota((n, 2 * LANES), 1) % LANES) // HALF_B
    w2[...] = jnp.zeros_like(w2)
    for q8 in range(GROUP_Q):
        w2[q8 * LANES:q8 * LANES + n, :] = jnp.where(lane_q == q8, cvt, 0.0).astype(BF)
    cv3 = dot32(cv, jnp.where(iota((v, half_cols), 0) == iota((v, half_cols), 1) % v, 1.0, 0.0).astype(BF)).astype(BF)
    chunk = 16 * 16
    mask3 = (iota((chunk, half_cols), 0) % HALF_B) == (iota((chunk, half_cols), 1) // v)

    def row_sel(c):
        return jnp.where(iota((chunk, n), 0) // 16 + 16 * c == iota((chunk, n), 1), 1.0, 0.0).astype(BF)

    for c in range(n // 16):
        w3[c * chunk:(c + 1) * chunk, :] = jnp.where(mask3, dot32(row_sel(c), cv3), 0.0).astype(BF)

    for a in range(v):
        evc[a:a + 1, :] = jnp.full((1, LANES), ev_s[a], F32)

    cot = cot_ref[...]
    pad = jnp.zeros((n, LANES - n), BF)

    def step1(p, t_ref, g_lo, g_hi):
        slot = p % 3
        for g in range(g_lo, g_hi):
            for k in range(GROUP_Q // 2):
                q = g * GROUP_Q + 2 * k
                w = jnp.concatenate([abuf[slot, q], pad, abuf[slot, q + 1], pad], axis=1)
                t_ref[g * o:(g + 1) * o, k * 2 * LANES:(k + 1) * 2 * LANES] = dot32(cot, w).astype(BF)

    def step2(t_ref, h_ref, g_lo, g_hi):
        res = dot32(t_ref[g_lo * o:g_hi * o, :], w2[...]).astype(BF)
        for g in range(g_lo, g_hi):
            for hi in range(nb_hi):
                h_ref[hi * o:(hi + 1) * o, g * LANES:(g + 1) * LANES] = (
                    res[(g - g_lo) * o:(g - g_lo + 1) * o, hi * LANES:(hi + 1) * LANES])

    def step3(p, h_ref):
        res = dot32(h_ref[...], w3[...]).astype(BF)
        for hi in range(nb_hi):
            for d in range(ndev):
                gbuf[p, d, :, hi * half_cols:(hi + 1) * half_cols] = (
                    res[hi * o + d * oj:hi * o + (d + 1) * oj, :])

    def send(p):
        for k, d in enumerate(peers):
            pltpu.make_async_remote_copy(
                src_ref=gbuf.at[p, d], dst_ref=recv.at[me * rows + p],
                send_sem=send_sem.at[k], recv_sem=recv_sem.at[k],
                device_id={"dev": d}, device_id_type=pl.DeviceIdType.MESH).start()
        recv[me * rows + p] = gbuf[p, me]

    tbufs, hbufs = (t0, t1), (h0, h1)
    cut = groups // 2

    def stage(t, par, s1=True, s2=True, s3=True, prefetch=True):
        if s1:
            a_copy(t).wait()
            if prefetch:
                a_copy(t + 2).start()
        for lo, hi in ((0, cut), (cut, groups)):
            if s1:
                step1(t, tbufs[par], lo, hi)
            if s2:
                step2(tbufs[1 - par], hbufs[1 - par], lo, hi)
        if s3:
            step3(t - 2, hbufs[par])

    stage(0, 0, s2=False, s3=False)
    stage(1, 1, s3=False)
    pl.semaphore_wait(barrier, 3)
    stage(2, 0)
    send(0)
    stage(3, 1)

    def pair(u, carry):
        t = 2 * u
        send(t - 3)
        stage(t, 0)
        send(t - 2)
        stage(t + 1, 1)
        return carry

    lax.fori_loop(2, rows // 2 - 1, pair, 0)
    send(rows - 5)
    stage(rows - 2, 0, prefetch=False)
    send(rows - 4)
    stage(rows - 1, 1, prefetch=False)
    send(rows - 3)
    stage(rows, 0, s1=False)
    send(rows - 2)
    stage(rows + 1, 1, s1=False, s2=False)
    send(rows - 1)

    lanes4 = oj * o
    cox = lax.dot_general(cot, jnp.where(iota((o, lanes4), 0) == iota((o, lanes4), 1) % o, 1.0, 0.0).astype(BF),
                          (((0,), (0,)), ((), ())), preferred_element_type=F32).astype(BF)
    mask4 = (iota((chunk, lanes4), 0) % 16) == (iota((chunk, lanes4), 1) // o)
    for c in range(n // 16):
        b4[c * chunk:(c + 1) * chunk, :] = jnp.where(mask4, dot32(row_sel(c), cox), 0.0).astype(BF)

    for k, d in enumerate(peers):
        whole = pltpu.make_async_remote_copy(
            src_ref=recv.at[pl.ds(me * rows, rows)], dst_ref=recv.at[pl.ds(d * rows, rows)],
            send_sem=send_sem.at[k], recv_sem=recv_sem.at[k],
            device_id={"dev": d}, device_id_type=pl.DeviceIdType.MESH)
        whole.wait_send()
        whole.wait_recv()

    g_all = recv.reshape(n * oj, v * v)
    b_per = 256 // v

    def step4(m, carry):
        cols = pl.ds(pl.multiple_of(m * 256, 256), 256)
        vm = lax.dot_general(g_all[:, cols], b4[...], (((0,), (0,)), ((), ())), preferred_element_type=F32)
        for b in range(b_per):
            base = pl.multiple_of((m * b_per + b) * PITCH, 8)
            for jt in range(lanes4 // LANES):
                vbuf[jt, pl.ds(base, v), :] = vm[b * v:(b + 1) * v, jt * LANES:(jt + 1) * LANES]
        return carry

    lax.fori_loop(0, v * v // 256, step4, 0)

    eo2 = jnp.concatenate([eo_ref[...], eo_ref[...]], axis=1)
    lane_lo = iota((1, LANES), 1) < o

    def step5(jt, carry):
        j0 = me * oj + 2 * jt
        eo_ji = jnp.where(lane_lo, eo_s[j0], eo_s[j0 + 1]) + eo2
        acc = jnp.zeros((8, LANES), F32)
        for b in range(v):
            eo_b = eo_ji - ev_s[b]
            for a in range(0, v, 8):
                x = vbuf[jt, b * PITCH + a:b * PITCH + a + 8, :]
                y = vbuf[jt, pl.ds(a * PITCH + b, 8, stride=PITCH), :]
                acc = acc + x * (2.0 * x - y) / (eo_b - evc[a:a + 8, :])
        tot = jnp.sum(acc, axis=0, keepdims=True)
        out_ref[pl.ds(2 * jt, 1), :] = tot[:, :o]
        out_ref[pl.ds(2 * jt + 1, 1), :] = tot[:, o:]
        return carry

    lax.fori_loop(0, lanes4 // LANES, step5, 0)


def solution(mesh):
    ndev = mesh.shape["dev"]

    def per_device(a_ints, c_occ, c_vir, eps_occ, eps_vir):
        rows, n = a_ints.shape[:2]
        o, v = c_occ.shape[1], c_vir.shape[1]
        oj = o // ndev
        vm = pl.BlockSpec(memory_space=pltpu.VMEM)
        sm = pl.BlockSpec(memory_space=pltpu.SMEM)
        e_t = pl.pallas_call(
            functools.partial(kernel, (rows, n, o, v, ndev)),
            out_shape=jax.ShapeDtypeStruct((oj, o), F32),
            in_specs=[sm, sm, vm, vm, vm, pl.BlockSpec(memory_space=pl.ANY)],
            out_specs=vm,
            scratch_shapes=[
                pltpu.VMEM((3, n, n, n), BF),
                pltpu.VMEM((n // GROUP_Q * o, GROUP_Q * LANES), BF),
                pltpu.VMEM((n // GROUP_Q * o, GROUP_Q * LANES), BF),
                pltpu.VMEM((v // HALF_B * o, n // GROUP_Q * LANES), BF),
                pltpu.VMEM((v // HALF_B * o, n // GROUP_Q * LANES), BF),
                pltpu.VMEM((GROUP_Q * LANES, 2 * LANES), BF),
                pltpu.VMEM((n * HALF_B, HALF_B * v), BF),
                pltpu.VMEM((n * oj, oj * o), BF),
                pltpu.VMEM((rows, ndev, oj, v * v), BF),
                pltpu.VMEM((n, oj, v * v), BF),
                pltpu.VMEM((oj * o // LANES, v * PITCH, LANES), F32),
                pltpu.VMEM((v, LANES), F32),
                pltpu.SemaphoreType.DMA((3,)),
                pltpu.SemaphoreType.DMA((3,)),
                pltpu.SemaphoreType.DMA((3,)),
            ],
            compiler_params=pltpu.CompilerParams(
                collective_id=0, has_side_effects=True, vmem_limit_bytes=60 * 2 ** 20),
            name="mp2",
        )(eps_occ, eps_vir, eps_occ[None, :], c_occ.T, c_vir, a_ints)
        return e_t.T

    return jax.shard_map(
        per_device,
        mesh=mesh,
        in_specs=(P(("frag", "dev")), P("frag"), P("frag"), P("frag"), P("frag")),
        out_specs=P("frag", "dev"),
        check_vma=False,
    )
```

```python
import functools

import jax
import jax.numpy as jnp
from jax import lax
from jax.experimental import pallas as pl
from jax.experimental.pallas import tpu as pltpu
from jax.sharding import PartitionSpec as P

BF = jnp.bfloat16
F32 = jnp.float32
LANES = 128
GROUP_Q = 8
HALF_B = 16
PITCH = 40
LATE = 4


def iota(shape, dim):
    return lax.broadcasted_iota(jnp.int32, shape, dim)


def dot32(a, b):
    return jnp.dot(a, b, preferred_element_type=F32)


def dot_t(a, b):
    return lax.dot_general(a, b, (((0,), (0,)), ((), ())), preferred_element_type=F32)


def kernel(dims, eo_s, ev_s, eo_ref, cot_ref, cvt_ref, a_hbm, out_ref,
           abuf, t0, t1, h0, h1, w2, w3, b4, gbuf, recv, gt, vbuf, evc,
           a_sem, send_sem, recv_sem):
    rows, n, o, v, ndev = dims
    oj = o // ndev
    groups = n // GROUP_Q
    nb_hi = v // HALF_B
    half_cols = HALF_B * v
    early = rows - LATE
    me = lax.axis_index("dev")
    partner = me + 1 - 2 * (me % 2)
    peers = ((me + 2) % 4, (partner + 2) % 4, partner)

    def a_copy(p):
        slot = p % 3
        return pltpu.make_async_copy(a_hbm.at[p], abuf.at[slot], a_sem.at[slot])

    a_copy(0).start()
    a_copy(1).start()

    barrier = pltpu.get_barrier_semaphore()
    for d in peers:
        pl.semaphore_signal(barrier, inc=1, device_id={"dev": d},
                            device_id_type=pl.DeviceIdType.MESH)

    cvt = cvt_ref[...]
    col_b = (iota((v, 2 * LANES), 1) // LANES) * HALF_B + iota((v, 2 * LANES), 1) % HALF_B
    cv2 = dot_t(cvt, jnp.where(iota((v, 2 * LANES), 0) == col_b, 1.0, 0.0).astype(BF))
    lane_q = (iota((n, 2 * LANES), 1) % LANES) // HALF_B
    w2[...] = jnp.zeros_like(w2)
    for q8 in range(GROUP_Q):
        w2[q8 * LANES:q8 * LANES + n, :] = jnp.where(lane_q == q8, cv2, 0.0).astype(BF)
    cv3 = dot_t(cvt, jnp.where(iota((v, half_cols), 0) == iota((v, half_cols), 1) % v, 1.0, 0.0).astype(BF)).astype(BF)
    chunk = 16 * 16
    mask3 = (iota((chunk, half_cols), 0) % HALF_B) == (iota((chunk, half_cols), 1) // v)
    for c in range(n // 16):
        sel = jnp.where(iota((chunk, n), 0) // HALF_B + 16 * c == iota((chunk, n), 1), 1.0, 0.0).astype(BF)
        w3[c * chunk:(c + 1) * chunk, :] = jnp.where(mask3, dot32(sel, cv3), 0.0).astype(BF)

    cot = cot_ref[...]
    pad = jnp.zeros((n, LANES - n), BF)

    def step1(p, t_ref, g_lo, g_hi):
        slot = p % 3
        for g in range(g_lo, g_hi):
            for k in range(GROUP_Q // 2):
                q = g * GROUP_Q + 2 * k
                w = jnp.concatenate([abuf[slot, q], pad, abuf[slot, q + 1], pad], axis=1)
                t_ref[g * o:(g + 1) * o, k * 2 * LANES:(k + 1) * 2 * LANES] = dot32(cot, w).astype(BF)

    def step2(t_ref, h_ref, g_lo, g_hi):
        res = dot32(t_ref[g_lo * o:g_hi * o, :], w2[...]).astype(BF)
        for g in range(g_lo, g_hi):
            for hi in range(nb_hi):
                h_ref[hi * o:(hi + 1) * o, g * LANES:(g + 1) * LANES] = (
                    res[(g - g_lo) * o:(g - g_lo + 1) * o, hi * LANES:(hi + 1) * LANES])

    def step3(p, h_ref):
        res = dot32(h_ref[...], w3[...]).astype(BF)
        for hi in range(nb_hi):
            for d in range(ndev):
                gbuf[p, d, :, hi * half_cols:(hi + 1) * half_cols] = (
                    res[hi * o + d * oj:hi * o + (d + 1) * oj, :])

    def send(p):
        for k, d in enumerate(peers):
            pltpu.make_async_remote_copy(
                src_ref=gbuf.at[p, d], dst_ref=recv.at[p, me],
                send_sem=send_sem.at[k], recv_sem=recv_sem.at[k, p // early],
                device_id={"dev": d}, device_id_type=pl.DeviceIdType.MESH).start()
        recv[p, me] = gbuf[p, me]

    tbufs, hbufs = (t0, t1), (h0, h1)
    cut = groups // 2
    halves = ((0, cut), (cut, groups))

    def stage(t, par, s1=True, s2=True, s3=True, out=True, prefetch=True):
        if s1:
            a_copy(t).wait()
            if prefetch:
                a_copy(t + 2).start()
        if out:
            send(t - 3)
        if s3:
            step3(t - 2, hbufs[par])
        for lo, hi in halves:
            if s1:
                step1(t, tbufs[par], lo, hi)
            if s2:
                step2(tbufs[1 - par], hbufs[1 - par], lo, hi)

    stage(0, 0, s2=False, s3=False, out=False)
    step2(t0, h0, 0, groups)
    step3(0, h0)
    a_copy(1).wait()
    a_copy(3).start()
    step1(1, t1, 0, cut)
    pl.semaphore_wait(barrier, 3)
    send(0)
    step1(1, t1, cut, groups)
    stage(2, 0, s3=False, out=False)
    stage(3, 1, out=False)

    def pair(u, carry):
        t = 2 * u
        stage(t, 0)
        stage(t + 1, 1)
        return carry

    lax.fori_loop(2, rows // 2 - 1, pair, 0)
    stage(rows - 2, 0, prefetch=False)
    stage(rows - 1, 1, prefetch=False)
    stage(rows, 0, s1=False)
    send(rows - 2)
    step3(rows - 1, h1)

    for a in range(v):
        evc[a:a + 1, :] = jnp.full((1, LANES), ev_s[a], F32)

    lanes4 = oj * o
    cox = dot_t(cot, jnp.where(iota((o, lanes4), 0) == iota((o, lanes4), 1) % o, 1.0, 0.0).astype(BF)).astype(BF)
    mask4 = (iota((chunk, lanes4), 0) % oj) == (iota((chunk, lanes4), 1) // o)
    per = ndev * oj
    for c in range(n // 16):
        if c == 1:
            send(rows - 1)
        p_all = ((iota((chunk, n), 0) // oj) % ndev) * rows + (chunk // per) * c + iota((chunk, n), 0) // per
        sel = jnp.where(p_all == iota((chunk, n), 1), 1.0, 0.0).astype(BF)
        b4[c * chunk:(c + 1) * chunk, :] = jnp.where(mask4, dot32(sel, cox), 0.0).astype(BF)

    def arrived(lo, count, which):
        for k, d in enumerate(peers):
            pltpu.make_async_remote_copy(
                src_ref=gbuf.at[pl.ds(lo, count), d], dst_ref=recv.at[pl.ds(lo, count), d],
                send_sem=send_sem.at[k], recv_sem=recv_sem.at[k, which],
                device_id={"dev": d}, device_id_type=pl.DeviceIdType.MESH).wait_recv()

    arrived(0, early, 0)
    g_all = recv.reshape(n * oj, v * v)
    k_early = early * per
    b_per = 256 // v

    def step4(m, carry):
        cols = pl.ds(pl.multiple_of(m * 256, 256), 256)
        vm = dot_t(g_all[0:k_early, cols], b4[0:k_early, :])
        for b in range(b_per):
            base = pl.multiple_of((m * b_per + b) * PITCH, 8)
            for jt in range(lanes4 // LANES):
                vbuf[jt, pl.ds(base, v), :] = vm[b * v:(b + 1) * v, jt * LANES:(jt + 1) * LANES]
        return carry

    lax.fori_loop(0, v * v // 256, step4, 0)
    arrived(early, LATE, 1)
    gt[...] = g_all[k_early:, :].T

    def step4_late(nt):
        vm = dot32(gt[...], b4[k_early:, nt * 256:(nt + 1) * 256])
        for b in range(v):
            for h in range(2):
                vbuf[2 * nt + h, b * PITCH:b * PITCH + v, :] += (
                    vm[b * v:(b + 1) * v, h * LANES:(h + 1) * LANES])

    eo2 = jnp.concatenate([eo_ref[...], eo_ref[...]], axis=1)
    lane_lo = iota((1, LANES), 1) < o

    def step5(jt):
        j0 = me * oj + 2 * jt
        eo_ji = jnp.where(lane_lo, eo_s[j0], eo_s[j0 + 1]) + eo2
        diag = jnp.zeros((8, LANES), F32)
        off = jnp.zeros((8, LANES), F32)
        for b in range(v):
            eo_b = eo_ji - ev_s[b]
            for a in range(b // 8 * 8, v, 8):
                x = vbuf[jt, b * PITCH + a:b * PITCH + a + 8, :]
                y = vbuf[jt, pl.ds(a * PITCH + b, 8, stride=PITCH), :]
                den = eo_b - evc[a:a + 8, :]
                if a == b // 8 * 8:
                    diag = diag + x * (2.0 * x - y) / den
                else:
                    off = off + (x * (x - y) + y * y) / den
        tot = jnp.sum(diag + 2.0 * off, axis=0, keepdims=True)
        out_ref[2 * jt:2 * jt + 1, :] = tot[:, :o]
        out_ref[2 * jt + 1:2 * jt + 2, :] = tot[:, o:]

    blocks = lanes4 // 256
    step4_late(0)
    for nt in range(blocks):
        if nt + 1 < blocks:
            step4_late(nt + 1)
        step5(2 * nt)
        step5(2 * nt + 1)

    for k, d in enumerate(peers):
        pltpu.make_async_remote_copy(
            src_ref=gbuf.at[:, d], dst_ref=recv.at[:, d],
            send_sem=send_sem.at[k], recv_sem=recv_sem.at[k, 0],
            device_id={"dev": d}, device_id_type=pl.DeviceIdType.MESH).wait_send()


def solution(mesh):
    ndev = mesh.shape["dev"]

    def per_device(a_ints, c_occ, c_vir, eps_occ, eps_vir):
        rows, n = a_ints.shape[:2]
        o, v = c_occ.shape[1], c_vir.shape[1]
        oj = o // ndev
        vm = pl.BlockSpec(memory_space=pltpu.VMEM)
        sm = pl.BlockSpec(memory_space=pltpu.SMEM)
        e_t = pl.pallas_call(
            functools.partial(kernel, (rows, n, o, v, ndev)),
            out_shape=jax.ShapeDtypeStruct((oj, o), F32),
            in_specs=[sm, sm, vm, vm, vm, pl.BlockSpec(memory_space=pl.ANY)],
            out_specs=vm,
            scratch_shapes=[
                pltpu.VMEM((3, n, n, n), BF),
                pltpu.VMEM((n // GROUP_Q * o, GROUP_Q * LANES), BF),
                pltpu.VMEM((n // GROUP_Q * o, GROUP_Q * LANES), BF),
                pltpu.VMEM((v // HALF_B * o, n // GROUP_Q * LANES), BF),
                pltpu.VMEM((v // HALF_B * o, n // GROUP_Q * LANES), BF),
                pltpu.VMEM((GROUP_Q * LANES, 2 * LANES), BF),
                pltpu.VMEM((n * HALF_B, HALF_B * v), BF),
                pltpu.VMEM((n * oj, oj * o), BF),
                pltpu.VMEM((rows, ndev, oj, v * v), BF),
                pltpu.VMEM((rows, ndev, oj, v * v), BF),
                pltpu.VMEM((v * v, LATE * ndev * oj), BF),
                pltpu.VMEM((oj * o // LANES, v * PITCH, LANES), F32),
                pltpu.VMEM((v, LANES), F32),
                pltpu.SemaphoreType.DMA((3,)),
                pltpu.SemaphoreType.DMA((3,)),
                pltpu.SemaphoreType.DMA((3, 2)),
            ],
            compiler_params=pltpu.CompilerParams(
                collective_id=0, has_side_effects=True, vmem_limit_bytes=60 * 2 ** 20),
            name="mp2",
        )(eps_occ, eps_vir, eps_occ[None, :], c_occ.T, c_vir.T, a_ints)
        return e_t.T

    return jax.shard_map(
        per_device,
        mesh=mesh,
        in_specs=(P(("frag", "dev")), P("frag"), P("frag"), P("frag"), P("frag")),
        out_specs=P("frag", "dev"),
        check_vma=False,
    )
```

```python
import functools

import jax
import jax.numpy as jnp
from jax import lax
from jax.experimental import pallas as pl
from jax.experimental.pallas import tpu as pltpu
from jax.sharding import PartitionSpec as P

BF = jnp.bfloat16
F32 = jnp.float32
LANES = 128
GROUP_Q = 8
B_LOW = 8
PITCH = 40
SLOTS = 4
LATE = 4


def iota(shape, dim):
    return lax.broadcasted_iota(jnp.int32, shape, dim)


def dot32(a, b):
    return jnp.dot(a, b, preferred_element_type=F32)


def dot_t(a, b):
    return lax.dot_general(a, b, (((0,), (0,)), ((), ())), preferred_element_type=F32)


def kernel(dims, eo_hbm, ev_hbm, cot_hbm, cvt_hbm, a_hbm, out_ref,
           eo_ref, ev_ref, cot_ref, cvt_ref, abuf, tbuf, hbuf, w2, w3, b4, gbuf, recv, gt, vbuf, rtab, eoj, evc, coxb,
           in_sem, a0_sem, a_sem, send_sem, recv_sem):
    rows, n, o, v, ndev = dims
    oj = o // ndev
    groups = n // GROUP_Q
    nb_hi = v // B_LOW
    blk = GROUP_Q * B_LOW
    cols3 = B_LOW * v
    early = rows - LATE
    lanes4 = oj * o
    me = lax.axis_index("dev")
    partner = me + 1 - 2 * (me % 2)
    peers = ((me + 2) % 4, (partner + 2) % 4, partner)

    def a_copy(p):
        slot = p % SLOTS
        return pltpu.make_async_copy(a_hbm.at[p], abuf.at[slot], a_sem.at[slot])

    pieces = [(g, min(g + 4, groups)) for g in range(0, groups, 4)]
    first = [pltpu.make_async_copy(a_hbm.at[0, pl.ds(lo * GROUP_Q, (hi - lo) * GROUP_Q)],
                                   abuf.at[0, pl.ds(lo * GROUP_Q, (hi - lo) * GROUP_Q)], a0_sem.at[i])
             for i, (lo, hi) in enumerate(pieces)]
    small = [pltpu.make_async_copy(src, dst, in_sem.at[i]) for i, (src, dst) in enumerate(
        ((cvt_hbm, cvt_ref), (cot_hbm, cot_ref), (eo_hbm, eo_ref), (ev_hbm, ev_ref)))]
    small[0].start()
    small[1].start()
    for c in first:
        c.start()
    small[2].start()
    small[3].start()

    barrier = pltpu.get_barrier_semaphore()
    for d in peers:
        pl.semaphore_signal(barrier, inc=1, device_id={"dev": d},
                            device_id_type=pl.DeviceIdType.MESH)

    small[0].wait()
    small[1].wait()
    cvt = cvt_ref[...]
    lane2 = iota((v, 2 * LANES), 1)
    col_b = lane2 // blk * B_LOW + lane2 % B_LOW
    cv2 = dot_t(cvt, jnp.where(iota((v, 2 * LANES), 0) == col_b, 1.0, 0.0).astype(BF))
    lane_q = iota((n, 2 * LANES), 1) % blk // B_LOW
    w2[...] = jnp.zeros_like(w2)
    for q8 in range(GROUP_Q):
        w2[q8 * LANES:q8 * LANES + n, :] = jnp.where(lane_q == q8, cv2, 0.0).astype(BF)
    cv3 = dot_t(cvt, jnp.where(iota((v, cols3), 0) == iota((v, cols3), 1) % v, 1.0, 0.0).astype(BF)).astype(BF)
    chunk = 256
    mask3 = (iota((LANES, cols3), 0) % B_LOW) == (iota((LANES, cols3), 1) // v)
    per3 = LANES // B_LOW
    for c in range(n // per3):
        sel = jnp.where(iota((LANES, n), 0) // B_LOW + per3 * c == iota((LANES, n), 1), 1.0, 0.0).astype(BF)
        w3[c * LANES:(c + 1) * LANES, :] = jnp.where(mask3, dot32(sel, cv3), 0.0).astype(BF)

    cot = cot_ref[...]
    pad = jnp.zeros((n, LANES - n), BF)

    def step1(p, g_lo, g_hi):
        slot = p % SLOTS
        for g in range(g_lo, g_hi):
            for k in range(GROUP_Q // 2):
                q = g * GROUP_Q + 2 * k
                w = jnp.concatenate([abuf[slot, q], pad, abuf[slot, q + 1], pad], axis=1)
                tbuf[g * o:(g + 1) * o, k * 2 * LANES:(k + 1) * 2 * LANES] = dot32(cot, w).astype(BF)

    def step2(g_lo, g_hi):
        res = dot32(tbuf[g_lo * o:g_hi * o, :], w2[...]).astype(BF)
        for g in range(g_lo, g_hi, 2):
            at = (g - g_lo) * o
            for hi in range(nb_hi):
                hbuf[hi * o:(hi + 1) * o, g * blk:(g + 2) * blk] = jnp.concatenate(
                    [res[at:at + o, hi * blk:(hi + 1) * blk], res[at + o:at + 2 * o, hi * blk:(hi + 1) * blk]], axis=1)

    def step3(p):
        res = dot32(hbuf[...], w3[...]).astype(BF)
        for hi in range(nb_hi):
            for d in range(ndev):
                gbuf[p, d, :, hi * cols3:(hi + 1) * cols3] = (
                    res[hi * o + d * oj:hi * o + (d + 1) * oj, :])

    def send(p):
        for k, d in enumerate(peers):
            pltpu.make_async_remote_copy(
                src_ref=gbuf.at[p, d], dst_ref=recv.at[p, me],
                send_sem=send_sem.at[k], recv_sem=recv_sem.at[k, p // early],
                device_id={"dev": d}, device_id_type=pl.DeviceIdType.MESH).start()

    def keep(p):
        recv[p, me] = gbuf[p, me]

    mask4 = (iota((chunk, lanes4), 0) % oj) == (iota((chunk, lanes4), 1) // o)
    per = ndev * oj

    def operand4(c):
        p_all = ((iota((chunk, n), 0) // oj) % ndev) * rows + (chunk // per) * c + iota((chunk, n), 0) // per
        sel = jnp.where(p_all == iota((chunk, n), 1), 1.0, 0.0).astype(BF)
        at = pl.ds(pl.multiple_of(c * chunk, chunk), chunk)
        b4[at, :] = jnp.where(mask4, dot32(sel, coxb[...]), 0.0).astype(BF)

    def recips(b):
        ev_b = evc[pl.ds(b, 1), :]
        at = pl.ds(pl.multiple_of(b * v, v), v)
        for jt in range(lanes4 // LANES):
            rtab[jt, at, :] = 1.0 / ((eoj[jt:jt + 1, :] - ev_b) - evc[...])

    cut = groups // 2 + 1

    def stage(t, out=True, extra=None):
        if out:
            send(t - 2)
            keep(t - 2)
        a_copy(t).wait()
        ahead = t + 2
        if isinstance(t, int):
            if ahead < rows:
                a_copy(ahead).start()
        else:
            @pl.when(ahead < rows)
            def _():
                a_copy(ahead).start()
        step2(cut, groups)
        step1(t, 0, cut)
        step3(t - 1)
        if extra is not None:
            extra()
        step1(t, cut, groups)
        step2(0, cut)

    for i, (lo, hi) in enumerate(pieces):
        first[i].wait()
        if i in (0, 2):
            a_copy(1 + i // 2).start()
        step1(0, lo, hi)
        if i > 0:
            step2(*pieces[i - 1])
    step2(*pieces[-1])
    step3(0)
    a_copy(1).wait()
    a_copy(3).start()
    step1(1, 0, 2)
    pl.semaphore_wait(barrier, 3)
    send(0)
    keep(0)
    step1(1, 2, groups)
    step2(0, cut)

    small[2].wait()
    small[3].wait()
    eo = eo_ref[...]
    eo2 = jnp.concatenate([eo, eo], axis=1)
    for jt in range(lanes4 // LANES):
        j0 = me * oj + 2 * jt
        lo, hi = (jnp.sum(jnp.where(iota((1, o), 1) == j0 + h, eo, 0.0), axis=1, keepdims=True) for h in range(2))
        eoj[jt:jt + 1, :] = jnp.where(iota((1, LANES), 1) < o, lo, hi) + eo2
    ev_col = jnp.sum(jnp.where(iota((v, v), 0) == iota((v, v), 1), ev_ref[...], 0.0), axis=1, keepdims=True)
    evc[...] = jnp.broadcast_to(ev_col, (v, LANES))
    coxb[...] = dot_t(cot, jnp.where(iota((o, lanes4), 0) == iota((o, lanes4), 1) % o, 1.0, 0.0).astype(BF)).astype(BF)

    stage(2, out=False)
    lo5 = 3 + n // 16
    hi5 = lo5 + v // 2

    def with_operand4(t, carry):
        stage(t, extra=lambda: operand4(t - 3))
        return carry

    def with_recips(t, carry):
        def both():
            recips(2 * (t - lo5))
            recips(2 * (t - lo5) + 1)
        stage(t, extra=both)
        return carry

    lax.fori_loop(3, lo5, with_operand4, 0)
    lax.fori_loop(lo5, hi5, with_recips, 0)
    for t in range(hi5, rows):
        stage(t)
    send(rows - 2)
    keep(rows - 2)
    step2(cut, groups)
    step3(rows - 1)
    keep(rows - 1)

    def arrived(lo, count, which):
        for k, d in enumerate(peers):
            pltpu.make_async_remote_copy(
                src_ref=gbuf.at[pl.ds(lo, count), d], dst_ref=recv.at[pl.ds(lo, count), d],
                send_sem=send_sem.at[k], recv_sem=recv_sem.at[k, which],
                device_id={"dev": d}, device_id_type=pl.DeviceIdType.MESH).wait_recv()

    send(rows - 1)
    arrived(0, early, 0)
    g_all = recv.reshape(n * oj, v * v)
    k_early = early * per
    b_per = 256 // v

    def step4(m, carry):
        cols = pl.ds(pl.multiple_of(m * 256, 256), 256)
        vm = dot_t(g_all[0:k_early, cols], b4[0:k_early, :])
        for b in range(b_per):
            base = pl.multiple_of((m * b_per + b) * PITCH, 8)
            for jt in range(lanes4 // LANES):
                vbuf[jt, pl.ds(base, v), :] = vm[b * v:(b + 1) * v, jt * LANES:(jt + 1) * LANES]
        return carry

    lax.fori_loop(0, v * v // 256, step4, 0)
    arrived(early, LATE, 1)
    gt[...] = g_all[k_early:, :].T

    def step4_late(nt):
        vm = dot32(gt[...], b4[k_early:, nt * 256:(nt + 1) * 256])
        for b in range(v):
            for h in range(2):
                vbuf[2 * nt + h, b * PITCH:b * PITCH + v, :] += (
                    vm[b * v:(b + 1) * v, h * LANES:(h + 1) * LANES])

    def step5(jt):
        diag = jnp.zeros((8, LANES), F32)
        off = jnp.zeros((8, LANES), F32)
        for b in range(v):
            for a in range(b // 8 * 8, v, 8):
                x = vbuf[jt, b * PITCH + a:b * PITCH + a + 8, :]
                y = vbuf[jt, pl.ds(a * PITCH + b, 8, stride=PITCH), :]
                r = rtab[jt, b * v + a:b * v + a + 8, :]
                if a == b // 8 * 8:
                    diag = diag + x * (2.0 * x - y) * r
                else:
                    off = off + (x * (x - y) + y * y) * r
        tot = jnp.sum(diag + 2.0 * off, axis=0, keepdims=True)
        out_ref[2 * jt:2 * jt + 1, :] = tot[:, :o]
        out_ref[2 * jt + 1:2 * jt + 2, :] = tot[:, o:]

    blocks = lanes4 // 256
    step4_late(0)
    for nt in range(blocks):
        if nt + 1 < blocks:
            step4_late(nt + 1)
        step5(2 * nt)
        step5(2 * nt + 1)

    for k, d in enumerate(peers):
        pltpu.make_async_remote_copy(
            src_ref=gbuf.at[:, d], dst_ref=recv.at[:, d],
            send_sem=send_sem.at[k], recv_sem=recv_sem.at[k, 0],
            device_id={"dev": d}, device_id_type=pl.DeviceIdType.MESH).wait_send()


def solution(mesh):
    ndev = mesh.shape["dev"]

    def per_device(a_ints, c_occ, c_vir, eps_occ, eps_vir):
        rows, n = a_ints.shape[:2]
        o, v = c_occ.shape[1], c_vir.shape[1]
        oj = o // ndev
        hbm = pl.BlockSpec(memory_space=pl.ANY)
        lanes4 = oj * o
        e_t = pl.pallas_call(
            functools.partial(kernel, (rows, n, o, v, ndev)),
            out_shape=jax.ShapeDtypeStruct((oj, o), F32),
            in_specs=[hbm] * 5,
            out_specs=pl.BlockSpec(memory_space=pltpu.VMEM),
            scratch_shapes=[
                pltpu.VMEM((1, o), F32),
                pltpu.VMEM((1, v), F32),
                pltpu.VMEM((o, n), BF),
                pltpu.VMEM((v, n), BF),
                pltpu.VMEM((SLOTS, n, n, n), BF),
                pltpu.VMEM((n // GROUP_Q * o, GROUP_Q * LANES), BF),
                pltpu.VMEM((v // B_LOW * o, n * B_LOW), BF),
                pltpu.VMEM((GROUP_Q * LANES, 2 * LANES), BF),
                pltpu.VMEM((n * B_LOW, B_LOW * v), BF),
                pltpu.VMEM((n * oj, lanes4), BF),
                pltpu.VMEM((rows, ndev, oj, v * v), BF),
                pltpu.VMEM((rows, ndev, oj, v * v), BF),
                pltpu.VMEM((v * v, LATE * ndev * oj), BF),
                pltpu.VMEM((lanes4 // LANES, v * PITCH, LANES), F32),
                pltpu.VMEM((lanes4 // LANES, v * v, LANES), F32),
                pltpu.VMEM((lanes4 // LANES, LANES), F32),
                pltpu.VMEM((v, LANES), F32),
                pltpu.VMEM((n, lanes4), BF),
                pltpu.SemaphoreType.DMA((4,)),
                pltpu.SemaphoreType.DMA((4,)),
                pltpu.SemaphoreType.DMA((SLOTS,)),
                pltpu.SemaphoreType.DMA((3,)),
                pltpu.SemaphoreType.DMA((3, 2)),
            ],
            compiler_params=pltpu.CompilerParams(
                collective_id=0, has_side_effects=True, vmem_limit_bytes=62 * 2 ** 20),
            name="mp2",
        )(eps_occ[None, :], eps_vir[None, :], c_occ.T, c_vir.T, a_ints)
        return e_t.T

    return jax.shard_map(
        per_device,
        mesh=mesh,
        in_specs=(P(("frag", "dev")), P("frag"), P("frag"), P("frag"), P("frag")),
        out_specs=P("frag", "dev"),
        check_vma=False,
    )
```

```python
import functools

import jax
import jax.numpy as jnp
from jax import lax
from jax.experimental import pallas as pl
from jax.experimental.pallas import tpu as pltpu
from jax.sharding import PartitionSpec as P

BF = jnp.bfloat16
F32 = jnp.float32
LANES = 128
GROUP_Q = 8
HALF_B = 16
PITCH = 40
LATE = 4


def iota(shape, dim):
    return lax.broadcasted_iota(jnp.int32, shape, dim)


def dot32(a, b):
    return jnp.dot(a, b, preferred_element_type=F32)


def dot_t(a, b):
    return lax.dot_general(a, b, (((0,), (0,)), ((), ())), preferred_element_type=F32)


def kernel(dims, eo_hbm, ev_hbm, cot_hbm, cvt_hbm, a_hbm, out_ref,
           eo_ref, ev_ref, cot_ref, cvt_ref, abuf, tbuf, hbuf, w2, w3, b4, gbuf, recv, gt, vbuf, rtab, eoj, evc, coxb,
           in_sem, a0_sem, a_sem, send_sem, recv_sem):
    rows, n, o, v, ndev = dims
    oj = o // ndev
    groups = n // GROUP_Q
    nb_hi = v // HALF_B
    half_cols = HALF_B * v
    early = rows - LATE
    lanes4 = oj * o
    me = lax.axis_index("dev")
    partner = me + 1 - 2 * (me % 2)
    peers = ((me + 2) % 4, (partner + 2) % 4, partner)

    def a_copy(p):
        slot = p % 3
        return pltpu.make_async_copy(a_hbm.at[p], abuf.at[slot], a_sem.at[slot])

    pieces = [(g, min(g + 4, groups)) for g in range(0, groups, 4)]
    first = [pltpu.make_async_copy(a_hbm.at[0, pl.ds(lo * GROUP_Q, (hi - lo) * GROUP_Q)],
                                   abuf.at[0, pl.ds(lo * GROUP_Q, (hi - lo) * GROUP_Q)], a0_sem.at[i])
             for i, (lo, hi) in enumerate(pieces)]
    small = [pltpu.make_async_copy(src, dst, in_sem.at[i]) for i, (src, dst) in enumerate(
        ((cvt_hbm, cvt_ref), (cot_hbm, cot_ref), (eo_hbm, eo_ref), (ev_hbm, ev_ref)))]
    small[0].start()
    small[1].start()
    for c in first:
        c.start()
    small[2].start()
    small[3].start()

    barrier = pltpu.get_barrier_semaphore()
    for d in peers:
        pl.semaphore_signal(barrier, inc=1, device_id={"dev": d},
                            device_id_type=pl.DeviceIdType.MESH)

    small[0].wait()
    small[1].wait()
    cvt = cvt_ref[...]
    col_b = (iota((v, 2 * LANES), 1) // LANES) * HALF_B + iota((v, 2 * LANES), 1) % HALF_B
    cv2 = dot_t(cvt, jnp.where(iota((v, 2 * LANES), 0) == col_b, 1.0, 0.0).astype(BF))
    lane_q = (iota((n, 2 * LANES), 1) % LANES) // HALF_B
    w2[...] = jnp.zeros_like(w2)
    for q8 in range(GROUP_Q):
        w2[q8 * LANES:q8 * LANES + n, :] = jnp.where(lane_q == q8, cv2, 0.0).astype(BF)
    cv3 = dot_t(cvt, jnp.where(iota((v, half_cols), 0) == iota((v, half_cols), 1) % v, 1.0, 0.0).astype(BF)).astype(BF)
    chunk = 16 * 16
    mask3 = (iota((chunk, half_cols), 0) % HALF_B) == (iota((chunk, half_cols), 1) // v)
    for c in range(n // 16):
        sel = jnp.where(iota((chunk, n), 0) // HALF_B + 16 * c == iota((chunk, n), 1), 1.0, 0.0).astype(BF)
        w3[c * chunk:(c + 1) * chunk, :] = jnp.where(mask3, dot32(sel, cv3), 0.0).astype(BF)

    cot = cot_ref[...]
    pad = jnp.zeros((n, LANES - n), BF)

    def step1(p, g_lo, g_hi):
        slot = p % 3
        for g in range(g_lo, g_hi):
            for k in range(GROUP_Q // 2):
                q = g * GROUP_Q + 2 * k
                w = jnp.concatenate([abuf[slot, q], pad, abuf[slot, q + 1], pad], axis=1)
                tbuf[g * o:(g + 1) * o, k * 2 * LANES:(k + 1) * 2 * LANES] = dot32(cot, w).astype(BF)

    def step2(g_lo, g_hi):
        res = dot32(tbuf[g_lo * o:g_hi * o, :], w2[...]).astype(BF)
        for g in range(g_lo, g_hi):
            for hi in range(nb_hi):
                hbuf[hi * o:(hi + 1) * o, g * LANES:(g + 1) * LANES] = (
                    res[(g - g_lo) * o:(g - g_lo + 1) * o, hi * LANES:(hi + 1) * LANES])

    def step3(p):
        res = dot32(hbuf[...], w3[...]).astype(BF)
        for hi in range(nb_hi):
            for d in range(ndev):
                gbuf[p, d, :, hi * half_cols:(hi + 1) * half_cols] = (
                    res[hi * o + d * oj:hi * o + (d + 1) * oj, :])

    def send(p):
        for k, d in enumerate(peers):
            pltpu.make_async_remote_copy(
                src_ref=gbuf.at[p, d], dst_ref=recv.at[p, me],
                send_sem=send_sem.at[k], recv_sem=recv_sem.at[k, p // early],
                device_id={"dev": d}, device_id_type=pl.DeviceIdType.MESH).start()
        recv[p, me] = gbuf[p, me]

    mask4 = (iota((chunk, lanes4), 0) % oj) == (iota((chunk, lanes4), 1) // o)
    per = ndev * oj

    def operand4(c):
        p_all = ((iota((chunk, n), 0) // oj) % ndev) * rows + (chunk // per) * c + iota((chunk, n), 0) // per
        sel = jnp.where(p_all == iota((chunk, n), 1), 1.0, 0.0).astype(BF)
        at = pl.ds(pl.multiple_of(c * chunk, chunk), chunk)
        b4[at, :] = jnp.where(mask4, dot32(sel, coxb[...]), 0.0).astype(BF)

    def recips(b):
        ev_b = evc[pl.ds(b, 1), :]
        at = pl.ds(pl.multiple_of(b * v, v), v)
        for jt in range(lanes4 // LANES):
            rtab[jt, at, :] = 1.0 / ((eoj[jt:jt + 1, :] - ev_b) - evc[...])

    cut = groups // 2

    def stage(t, s1=True, out=True, prefetch=True, extra=None):
        if s1:
            a_copy(t).wait()
            if prefetch:
                a_copy(t + 2).start()
        if out:
            send(t - 2)
        step2(cut, groups)
        if s1:
            step1(t, 0, cut)
        step3(t - 1)
        if extra is not None:
            extra()
        if s1:
            step2(0, cut)
            step1(t, cut, groups)

    for i, (lo, hi) in enumerate(pieces):
        first[i].wait()
        if i in (0, 2):
            a_copy(1 + i // 2).start()
        step1(0, lo, hi)
        if i > 0:
            step2(*pieces[i - 1])
    step2(*pieces[-1])
    step3(0)
    a_copy(1).wait()
    a_copy(3).start()
    step1(1, 0, 2)
    pl.semaphore_wait(barrier, 3)
    send(0)
    step1(1, 2, cut)
    step2(0, cut)
    step1(1, cut, groups)

    small[2].wait()
    small[3].wait()
    eo = eo_ref[...]
    eo2 = jnp.concatenate([eo, eo], axis=1)
    for jt in range(lanes4 // LANES):
        j0 = me * oj + 2 * jt
        lo, hi = (jnp.sum(jnp.where(iota((1, o), 1) == j0 + h, eo, 0.0), axis=1, keepdims=True) for h in range(2))
        eoj[jt:jt + 1, :] = jnp.where(iota((1, LANES), 1) < o, lo, hi) + eo2
    ev_col = jnp.sum(jnp.where(iota((v, v), 0) == iota((v, v), 1), ev_ref[...], 0.0), axis=1, keepdims=True)
    evc[...] = jnp.broadcast_to(ev_col, (v, LANES))
    coxb[...] = dot_t(cot, jnp.where(iota((o, lanes4), 0) == iota((o, lanes4), 1) % o, 1.0, 0.0).astype(BF)).astype(BF)

    stage(2, out=False)

    def with_operand4(t, carry):
        stage(t, extra=lambda: operand4(t - 3))
        return carry

    def with_recips(t, carry):
        def both():
            recips(2 * (t - lo5))
            recips(2 * (t - lo5) + 1)
        stage(t, extra=both)
        return carry

    lo5 = 3 + n // 16
    hi5 = lo5 + v // 2
    lax.fori_loop(3, lo5, with_operand4, 0)
    lax.fori_loop(lo5, hi5, with_recips, 0)
    for t in range(hi5, rows):
        stage(t, prefetch=t + 2 < rows)
    stage(rows, s1=False)

    def arrived(lo, count, which):
        for k, d in enumerate(peers):
            pltpu.make_async_remote_copy(
                src_ref=gbuf.at[pl.ds(lo, count), d], dst_ref=recv.at[pl.ds(lo, count), d],
                send_sem=send_sem.at[k], recv_sem=recv_sem.at[k, which],
                device_id={"dev": d}, device_id_type=pl.DeviceIdType.MESH).wait_recv()

    send(rows - 1)
    arrived(0, early, 0)
    g_all = recv.reshape(n * oj, v * v)
    k_early = early * per
    b_per = 256 // v

    def step4(m, carry):
        cols = pl.ds(pl.multiple_of(m * 256, 256), 256)
        vm = dot_t(g_all[0:k_early, cols], b4[0:k_early, :])
        for b in range(b_per):
            base = pl.multiple_of((m * b_per + b) * PITCH, 8)
            for jt in range(lanes4 // LANES):
                vbuf[jt, pl.ds(base, v), :] = vm[b * v:(b + 1) * v, jt * LANES:(jt + 1) * LANES]
        return carry

    lax.fori_loop(0, v * v // 256, step4, 0)
    arrived(early, LATE, 1)
    gt[...] = g_all[k_early:, :].T

    def step4_late(nt):
        vm = dot32(gt[...], b4[k_early:, nt * 256:(nt + 1) * 256])
        for b in range(v):
            for h in range(2):
                vbuf[2 * nt + h, b * PITCH:b * PITCH + v, :] += (
                    vm[b * v:(b + 1) * v, h * LANES:(h + 1) * LANES])

    def step5(jt):
        diag = jnp.zeros((8, LANES), F32)
        off = jnp.zeros((8, LANES), F32)
        for b in range(v):
            for a in range(b // 8 * 8, v, 8):
                x = vbuf[jt, b * PITCH + a:b * PITCH + a + 8, :]
                y = vbuf[jt, pl.ds(a * PITCH + b, 8, stride=PITCH), :]
                r = rtab[jt, b * v + a:b * v + a + 8, :]
                if a == b // 8 * 8:
                    diag = diag + x * (2.0 * x - y) * r
                else:
                    off = off + (x * (x - y) + y * y) * r
        tot = jnp.sum(diag + 2.0 * off, axis=0, keepdims=True)
        out_ref[2 * jt:2 * jt + 1, :] = tot[:, :o]
        out_ref[2 * jt + 1:2 * jt + 2, :] = tot[:, o:]

    blocks = lanes4 // 256
    step4_late(0)
    for nt in range(blocks):
        if nt + 1 < blocks:
            step4_late(nt + 1)
        step5(2 * nt)
        step5(2 * nt + 1)

    for k, d in enumerate(peers):
        pltpu.make_async_remote_copy(
            src_ref=gbuf.at[:, d], dst_ref=recv.at[:, d],
            send_sem=send_sem.at[k], recv_sem=recv_sem.at[k, 0],
            device_id={"dev": d}, device_id_type=pl.DeviceIdType.MESH).wait_send()


def solution(mesh):
    ndev = mesh.shape["dev"]

    def per_device(a_ints, c_occ, c_vir, eps_occ, eps_vir):
        rows, n = a_ints.shape[:2]
        o, v = c_occ.shape[1], c_vir.shape[1]
        oj = o // ndev
        hbm = pl.BlockSpec(memory_space=pl.ANY)
        lanes4 = oj * o
        e_t = pl.pallas_call(
            functools.partial(kernel, (rows, n, o, v, ndev)),
            out_shape=jax.ShapeDtypeStruct((oj, o), F32),
            in_specs=[hbm] * 5,
            out_specs=pl.BlockSpec(memory_space=pltpu.VMEM),
            scratch_shapes=[
                pltpu.VMEM((1, o), F32),
                pltpu.VMEM((1, v), F32),
                pltpu.VMEM((o, n), BF),
                pltpu.VMEM((v, n), BF),
                pltpu.VMEM((3, n, n, n), BF),
                pltpu.VMEM((n // GROUP_Q * o, GROUP_Q * LANES), BF),
                pltpu.VMEM((v // HALF_B * o, n // GROUP_Q * LANES), BF),
                pltpu.VMEM((GROUP_Q * LANES, 2 * LANES), BF),
                pltpu.VMEM((n * HALF_B, HALF_B * v), BF),
                pltpu.VMEM((n * oj, lanes4), BF),
                pltpu.VMEM((rows, ndev, oj, v * v), BF),
                pltpu.VMEM((rows, ndev, oj, v * v), BF),
                pltpu.VMEM((v * v, LATE * ndev * oj), BF),
                pltpu.VMEM((lanes4 // LANES, v * PITCH, LANES), F32),
                pltpu.VMEM((lanes4 // LANES, v * v, LANES), F32),
                pltpu.VMEM((lanes4 // LANES, LANES), F32),
                pltpu.VMEM((v, LANES), F32),
                pltpu.VMEM((n, lanes4), BF),
                pltpu.SemaphoreType.DMA((4,)),
                pltpu.SemaphoreType.DMA((4,)),
                pltpu.SemaphoreType.DMA((3,)),
                pltpu.SemaphoreType.DMA((3,)),
                pltpu.SemaphoreType.DMA((3, 2)),
            ],
            compiler_params=pltpu.CompilerParams(
                collective_id=0, has_side_effects=True, vmem_limit_bytes=60 * 2 ** 20),
            name="mp2",
        )(eps_occ[None, :], eps_vir[None, :], c_occ.T, c_vir.T, a_ints)
        return e_t.T

    return jax.shard_map(
        per_device,
        mesh=mesh,
        in_specs=(P(("frag", "dev")), P("frag"), P("frag"), P("frag"), P("frag")),
        out_specs=P("frag", "dev"),
        check_vma=False,
    )
```
